32 devices in a mesh: row: 8 (over z, x), col: 4 (over y, core).
Axes of the slice: x: 2, y: 2, z: 4, core: 2. Of those that a mesh axis runs over, the one named last changes fastest.
Arguments:
- voltage: float32 [2, 4096, 16384], P(None, ('row', 'col')), may hold values from -6 to 6
- chirp_phase: float32 [16384, 4096], P(('row', 'col')), may hold values from -3.140625 to 3.140625
- filter_taps: float32 [8, 1024], replicated, may hold values from -0.0625 to 0.0625
Outputs:
- filterbank: float32 [2, 1024, 65536], P(None, None, ('row', 'col'))
The draws below stay inside these ranges and needn't reach their ends.
All inputs are finite; a program needn't handle non-finite values.
Results may differ from the reference program's by a relative error of at most 0.00015.
Values sent between devices are 32-bit elements; how exact they have to be, the bound alone decides.
A program may use at most 192 MiB of HBM per device.

```python
import jax
import jax.numpy as jnp
from jax import lax

FFT_ROWS = 4096
FFT_COLS = 16384
CHANNELS = 1024
TAPS = 8
SPECTRA = 65536


def shard_levels(stream_key, shape, pieces, smallest, high):
    gain, own = 1.0, jax.random.fold_in(stream_key, 6)
    for axis_at, blocks in pieces:
        steps = jnp.exp(jax.random.uniform(jax.random.fold_in(own, axis_at), (blocks,), jnp.float32, smallest / len(pieces), high / len(pieces)))
        gain = gain * jnp.repeat(steps, shape[axis_at] // blocks).reshape([-1 if axis == axis_at else 1 for axis in range(len(shape))])
    return gain


def centred(key, extent, spread, bound, pieces=(), dtype=jnp.bfloat16):
    result = jax.random.normal(key, extent, jnp.float32) * spread
    if len(pieces) > 0:
        result = shard_levels(key, extent, pieces, -0.22, 0.18) * result
    return jnp.clip(result, min=-bound, max=bound).astype(dtype)


def setup_inputs(seed: int = 0) -> dict:
    key_list = jax.random.split(jax.random.key(seed), 4)
    return {
        "voltage": centred(key_list[0], (2, FFT_ROWS, FFT_COLS), 1.0, 6.0, ((1, 32),), jnp.float32),
        "chirp_phase": jnp.clip(jax.random.uniform(key_list[1], (FFT_COLS, FFT_ROWS), jnp.float32, -3.140625, 3.140625), -3.140625, 3.140625),
        "filter_taps": centred(key_list[2], (TAPS, CHANNELS), (TAPS * CHANNELS) ** -0.5, 0.0625, (), jnp.float32),
    }


def reference(voltage, chirp_phase, filter_taps):
    series = lax.complex(voltage[0], voltage[1]).reshape(-1)
    spectrum = jnp.fft.fft(series)
    rotation = lax.complex(jnp.cos(chirp_phase), jnp.sin(chirp_phase)).reshape(-1)
    cleaned = jnp.fft.ifft(spectrum * rotation)
    frames = cleaned.reshape(SPECTRA, CHANNELS)
    padded = jnp.pad(frames, ((TAPS - 1, 0), (0, 0)))
    weighted = jnp.zeros_like(frames)
    for tap_delay in range(TAPS):
        offset = TAPS - 1 - tap_delay
        weighted = weighted + filter_taps[tap_delay] * padded[offset:offset + SPECTRA]
    channels_out = jnp.fft.fft(weighted, axis=1)
    return jnp.stack([jnp.real(channels_out).T, jnp.imag(channels_out).T])
```

```python
import math

import jax
import jax.numpy as jnp
from jax import lax
from jax.sharding import PartitionSpec as P

precise = lax.Precision.HIGH


def passed_along(block, axis, distance):
    devices = range(lax.axis_size(axis))
    route = [(i - distance, i) for i in devices if i - distance in devices]
    return lax.ppermute(block, axis, route)


def dft_table(radix, direction):
    digits = jnp.arange(radix, dtype=jnp.int32)
    product = digits[:, None] * digits[None, :] % radix
    turn = direction * 2.0 * math.pi / radix * product.astype(jnp.float32)
    cos_part = jnp.cos(turn)
    sin_part = jnp.sin(turn)
    upper = jnp.stack([cos_part, sin_part], axis=1)
    lower = jnp.stack([-sin_part, cos_part], axis=1)
    return jnp.stack([upper, lower], axis=0)


def complex_product(values, cos_part, sin_part):
    real_part = values[0] * cos_part - values[1] * sin_part
    imag_part = values[0] * sin_part + values[1] * cos_part
    return jnp.stack([real_part, imag_part])


def inner_twist(outer_radix, inner_radix, direction):
    outer_digits = jnp.arange(outer_radix, dtype=jnp.int32)
    inner_digits = jnp.arange(inner_radix, dtype=jnp.int32)
    length = outer_radix * inner_radix
    product = outer_digits[:, None] * inner_digits[None, :] % length
    turn = direction * 2.0 * math.pi / length * product.astype(jnp.float32)
    return (jnp.cos(turn), jnp.sin(turn))


def dft_rows(values, direction):
    length = values.shape[1]
    column_count = values.shape[2]
    inner_radix = min(length, 128)
    outer_radix = length // inner_radix
    blocked = values.reshape(2, outer_radix, inner_radix, column_count)
    partial_value = jnp.einsum(
        "cadk,cabm->dkbm", dft_table(outer_radix, direction), blocked, precision=precise
    )
    cos_part, sin_part = inner_twist(outer_radix, inner_radix, direction)
    partial_value = complex_product(partial_value, cos_part[:, :, None], sin_part[:, :, None])
    result = jnp.einsum(
        "cbdq,ckbm->dqkm", dft_table(inner_radix, direction), partial_value, precision=precise
    )
    return result.reshape(2, length, column_count)


def dft_cols(values, direction):
    length = values.shape[2]
    row_count = values.shape[1]
    inner_radix = min(length, 128)
    outer_radix = length // inner_radix
    blocked = values.reshape(2, row_count, outer_radix, inner_radix)
    partial_value = jnp.einsum(
        "cadk,cmab->dmkb", dft_table(outer_radix, direction), blocked, precision=precise
    )
    cos_part, sin_part = inner_twist(outer_radix, inner_radix, direction)
    partial_value = complex_product(partial_value, cos_part, sin_part)
    result = jnp.einsum(
        "cbdq,cmkb->dmqk", dft_table(inner_radix, direction), partial_value, precision=precise
    )
    return result.reshape(2, row_count, length)


def unit_table(left_index, right_index, total, direction, factor):
    product = left_index[:, None] * right_index[None, :] % total
    turn = direction * 2.0 * math.pi / total * product.astype(jnp.float32)
    return factor * jnp.cos(turn), factor * jnp.sin(turn)


def rotate(values, row_start, row_count, col_start, col_count, total, direction, factor):
    split_rows = row_count >= col_count
    long_count = row_count if split_rows else col_count
    long_start = row_start if split_rows else col_start
    short_count = col_count if split_rows else row_count
    short_start = col_start if split_rows else row_start
    fine = min(long_count, 128)
    short_index = short_start + jnp.arange(short_count, dtype=jnp.int32)
    coarse_index = long_start + fine * jnp.arange(long_count // fine, dtype=jnp.int32)
    fine_index = jnp.arange(fine, dtype=jnp.int32)
    tables = (
        unit_table(coarse_index, short_index, total, direction, factor),
        unit_table(fine_index, short_index, total, direction, 1.0),
    )
    if split_rows:
        blocked = values.reshape(2, long_count // fine, fine, short_count)
        (cc, cs), (fc, fs) = tables
        cc, cs, fc, fs = cc[:, None, :], cs[:, None, :], fc[None], fs[None]
    else:
        blocked = values.reshape(2, short_count, long_count // fine, fine)
        (cc, cs), (fc, fs) = tables
        cc, cs = cc.T[:, :, None], cs.T[:, :, None]
        fc, fs = fc.T[:, None, :], fs.T[:, None, :]
    turned = complex_product(blocked, cc * fc - cs * fs, cc * fs + cs * fc)
    return turned.reshape(values.shape)


def unit_phase(phase):
    half = 0.5 * phase
    square = half * half
    sine = half * polynomial(square, (1, -6, 120, -5040, 362880, -39916800, 6227020800))
    cosine = polynomial(square, (1, -2, 24, -720, 40320, -3628800, 479001600))
    return 1.0 - 2.0 * sine * sine, 2.0 * sine * cosine


def polynomial(square, factorials):
    result = jnp.full_like(square, 1.0 / factorials[-1])
    for factorial in factorials[-2::-1]:
        result = result * square + 1.0 / factorial
    return result


def spread(values):
    return lax.all_to_all(values, ("row", "col"), split_axis=2, concat_axis=1, tiled=True)


def collect(values):
    return lax.all_to_all(values, ("row", "col"), split_axis=1, concat_axis=2, tiled=True)


def local(voltage, chirp_phase, filter_taps):
    device_count = lax.axis_size("row") * lax.axis_size("col")
    device = lax.axis_index(("row", "col"))
    local_rows = voltage.shape[1]
    total_rows = local_rows * device_count
    total_cols = voltage.shape[2]
    local_cols = total_cols // device_count
    total = total_rows * total_cols
    signal = spread(voltage)
    signal = dft_rows(signal, -1.0)
    signal = rotate(
        signal, 0, total_rows, device * local_cols, local_cols, total, -1.0, 1.0
    )
    signal = collect(signal)
    signal = dft_cols(signal, -1.0)
    turned_phase = jnp.transpose(chirp_phase)
    local_phase = lax.all_to_all(
        turned_phase, ("row", "col"), split_axis=0, concat_axis=1, tiled=True
    )
    signal = complex_product(signal, *unit_phase(local_phase))
    signal = dft_cols(signal, 1.0)
    signal = rotate(
        signal, device * local_rows, local_rows, 0, total_cols, total, 1.0, 1.0 / total
    )
    signal = spread(signal)
    signal = dft_rows(signal, 1.0)
    signal = collect(signal)
    tap_count = filter_taps.shape[0]
    channel_count = filter_taps.shape[1]
    samples = signal.reshape(2, local_rows * total_cols)
    frame_count = samples.shape[1] // channel_count
    frames = samples.reshape(2, frame_count, channel_count)
    history = passed_along(frames[:, frame_count - tap_count + 1 :, :], ("row", "col"), 1)
    extended = jnp.concatenate([history, frames], axis=1)
    turned = jnp.transpose(extended, (0, 2, 1))
    weighted = jnp.zeros((2, channel_count, frame_count), jnp.float32)
    for tap_delay in range(tap_count):
        offset = tap_count - 1 - tap_delay
        weighted = (
            weighted
            + filter_taps[tap_delay][None, :, None] * turned[:, :, offset : offset + frame_count]
        )
    return dft_rows(weighted, -1.0)


def solution(mesh):
    in_specs = (P(None, ("row", "col"), None), P(("row", "col"), None), P())
    out_specs = P(None, None, ("row", "col"))
    return jax.shard_map(local, mesh=mesh, in_specs=in_specs, out_specs=out_specs, check_vma=False)
```
